512 devices in a mesh: ctx: 64 (over y_lo, z, x), head: 8 (over y_hi, core).
Axes of the slice: x: 4, y: 8 (y_hi: 4, y_lo: 2; y = y_hi * 2 + y_lo), z: 8, core: 2. Of those that a mesh axis runs over, the one named last changes fastest.
Arguments:
- patches: bfloat16 [8192, 1280], P('ctx'), may hold values from -6 to 6
- patch_count: int32 [64], P('ctx'), may hold values from 1 to 128, as said below
- token_patch: int32 [8192], P('ctx'), may hold values from -1 to 127, as said below
- window_ids: int32 [8192], P('ctx'), may hold values from 1 to 8192, as said below
- text_embed: bfloat16 [8192, 4096], P('ctx', 'head'), may hold values from -200 to 200
- vit_norm_gain: float32 [1280], replicated, may hold values from 0.25 to 1.75
- vit_qkv: bfloat16 [1280, 3840], P(None, 'head'), may hold values from -0.15625 to 0.15625
- vit_qkv_bias: float32 [3840], P('head'), may hold values from -16 to 16
- vit_proj: bfloat16 [1280, 1280], P('head'), may hold values from -0.15625 to 0.15625
- vit_proj_bias: float32 [1280], replicated, may hold values from -1 to 1
- merge_norm_gain: float32 [1280], replicated, may hold values from 0.25 to 1.75
- merger: bfloat16 [1280, 4096], P('ctx', 'head'), may hold values from -0.15625 to 0.15625
- merger_bias: float32 [4096], P('head'), may hold values from -1 to 1
- llm_norm_gain: float32 [4096], replicated, may hold values from 0.25 to 1.75
- w_qkv: bfloat16 [4096, 6144], P('ctx', 'head'), may hold values from -0.09375 to 0.09375
- qkv_bias: float32 [6144], P('head'), may hold values from -16 to 16
Outputs:
- context: bfloat16 [8192, 4096], P('ctx', 'head')
The draws below stay inside these ranges and needn't reach their ends.
Inputs may be any that keep to these rules, and one draw needn't show every extreme that they name: `patch_count`: at most 128 live slots on one ctx index, reached by some index in every draw. `token_patch`: among the tokens of one ctx index, each live slot 0 to patch_count - 1 of that index appears exactly once; all other tokens hold -1. `window_ids`: ids never fall along the slots; a window lies within the slots of one ctx index and holds at most 64 consecutive slots; some window holds exactly 64.
All inputs are finite; a program needn't handle non-finite values.
Results may differ from the reference program's by a relative error of at most 0.012.
The reference program's roundings to bfloat16 on the way count: a program that leaves them out, or rounds other values in their place, can miss the bound.
Values may be sent and summed in bfloat16 or wider, within the bound.
A program may use at most 64 MiB of HBM per device.

```python
import math
import jax
import jax.numpy as jnp
from jax import lax

DV = 1280
VH = 16
VHD = 80
KVH = 8
HD = 128
D = 4096
QH = 4
WIN = 64
TOK_DEV = 128
TOKENS = 8192
N_CTX = 64


def shard_counts(key):
    shards = TOKENS // TOK_DEV
    base = jax.random.fold_in(key, 11)
    first = jax.random.randint(jax.random.fold_in(base, 1), (shards,), 1, TOK_DEV + 1)
    second = jax.random.randint(jax.random.fold_in(base, 2), (shards,), 1, TOK_DEV + 1)
    counts = jnp.minimum(first, second)
    fullest = jax.random.randint(jax.random.fold_in(base, 3), (), 0, shards)
    return jnp.where(jnp.arange(shards) == fullest, TOK_DEV, counts).astype(jnp.int32)


def draw_patch_count(key, part):
    return shard_counts(key)


def draw_token_patch(key, part):
    shards = TOKENS // TOK_DEV
    counts = shard_counts(key)
    shard_keys = jax.random.split(jax.random.fold_in(key, 12), shards)
    orders = jax.vmap(lambda one_key: jax.random.permutation(one_key, TOK_DEV))(shard_keys)
    chosen_slots = jnp.where(orders < counts[:, None], orders, -1)
    return chosen_slots.reshape(TOKENS).astype(jnp.int32)


def draw_window_ids(key, part):
    shards = TOKENS // TOK_DEV
    base = jax.random.fold_in(key, 13)
    marks = jax.random.randint(base, (shards, TOK_DEV), 0, 12) == 0
    local = jnp.arange(TOK_DEV)
    bounds = local % WIN == 0
    chosen = jax.random.randint(jax.random.fold_in(base, 1), (), 0, shards)
    quiet = (jnp.arange(shards)[:, None] == chosen) & (local[None, :] < WIN)
    marks = marks & jnp.logical_not(quiet) | bounds[None, :]
    window_numbers = jnp.cumsum(marks.astype(jnp.int32), axis=1) + jnp.arange(shards, dtype=jnp.int32)[:, None] * TOK_DEV
    return window_numbers.reshape(TOKENS).astype(jnp.int32)


def draw_text_embed(key, part):
    base = jax.random.fold_in(key, 14)
    row_scale = jnp.exp(jax.random.uniform(jax.random.fold_in(base, 1), (TOKENS, 1), minval=0.0, maxval=math.log(10.0)))
    column_rise = jnp.exp(jnp.linspace(0.0, math.log(3.0), D))[None, :] * jax.random.uniform(jax.random.fold_in(base, 2), (1, D), minval=0.5, maxval=1.5)
    values = jax.random.truncated_normal(jax.random.fold_in(base, 5), -4.0, 4.0, (TOKENS, D)) * row_scale * column_rise
    return values.astype(jnp.float32).astype(jnp.bfloat16)


def drawn_bias(base, heads, parts, head_size):
    drawn = jax.random.truncated_normal(jax.random.fold_in(base, 1), -3.0, 3.0, (heads, parts, head_size))
    values = drawn * 0.5
    return values.reshape(heads * parts * head_size).astype(jnp.float32)


def draw_vit_qkv_bias(key, part):
    return drawn_bias(jax.random.fold_in(key, 21), VH, 3, VHD)


def draw_qkv_bias(key, part):
    return drawn_bias(jax.random.fold_in(key, 22), KVH, QH + 2, HD)


def levels(key, shape, cuts, smallest, largest):
    def one(axis_at, shards_of):
        draws = jax.random.uniform(jax.random.fold_in(jax.random.fold_in(key, 6), axis_at), (shards_of,), jnp.float32, smallest / len(cuts), largest / len(cuts))
        return jnp.repeat(jnp.exp(draws), shape[axis_at] // shards_of).reshape((-1,) + (1,) * (len(shape) - axis_at - 1))

    level = one(*cuts[0])
    for cut in cuts[1:]:
        level = level * one(*cut)
    return level


def bell_draw(stream_key, extent, width, reach, cuts=(), held_as=jnp.bfloat16):
    values = jax.random.normal(stream_key, extent, jnp.float32) * width
    if len(cuts) > 0:
        values = levels(stream_key, extent, cuts, -0.22, 0.18) * values
    return jnp.clip(values, min=-reach, max=reach).astype(held_as)


def setup_inputs(seed: int = 0) -> dict:
    streams_of = jax.random.split(jax.random.key(seed), 17)
    patches = bell_draw(streams_of[0], (TOKENS, DV), 1.0, 6.0, ((0, 64),))
    patch_count = draw_patch_count(jax.random.fold_in(streams_of[16], 71), 0)
    token_patch = draw_token_patch(jax.random.fold_in(streams_of[16], 71), 0)
    window_ids = draw_window_ids(jax.random.fold_in(streams_of[16], 71), 0)
    text_embed = draw_text_embed(jax.random.fold_in(streams_of[16], 71), 0)
    vit_norm_gain = jnp.clip(1.0 + 0.15 * jax.random.normal(streams_of[5], (DV,), jnp.float32), 0.25, 1.75)
    vit_qkv = bell_draw(streams_of[6], (DV, 3 * DV), DV ** -0.5, 0.15625, ((1, 8),))
    vit_qkv_bias = draw_vit_qkv_bias(jax.random.fold_in(streams_of[16], 71), 0)
    vit_proj = bell_draw(streams_of[8], (DV, DV), DV ** -0.5, 0.15625, ((0, 8),))
    vit_proj_bias = jnp.clip(jax.random.uniform(streams_of[9], (DV,), jnp.float32, -1.0, 1.0), -1.0, 1.0)
    merge_norm_gain = jnp.clip(1.0 + 0.15 * jax.random.normal(streams_of[10], (DV,), jnp.float32), 0.25, 1.75)
    merger = bell_draw(streams_of[11], (DV, D), DV ** -0.5, 0.15625, ((0, 64), (1, 8)))
    merger_bias = jnp.clip(jax.random.uniform(streams_of[12], (D,), jnp.float32, -1.0, 1.0) * levels(streams_of[12], (D,), ((0, 8),), -0.4, 0.0), -1.0, 1.0)
    llm_norm_gain = jnp.clip(1.0 + 0.15 * jax.random.normal(streams_of[13], (D,), jnp.float32), 0.25, 1.75)
    w_qkv = bell_draw(streams_of[14], (D, KVH * (QH + 2) * HD), D ** -0.5, 0.09375, ((0, 64), (1, 8)))
    qkv_bias = draw_qkv_bias(jax.random.fold_in(streams_of[16], 71), 0)
    return dict(patches=patches, patch_count=patch_count, token_patch=token_patch, window_ids=window_ids, text_embed=text_embed, vit_norm_gain=vit_norm_gain, vit_qkv=vit_qkv, vit_qkv_bias=vit_qkv_bias, vit_proj=vit_proj, vit_proj_bias=vit_proj_bias, merge_norm_gain=merge_norm_gain, merger=merger, merger_bias=merger_bias, llm_norm_gain=llm_norm_gain, w_qkv=w_qkv, qkv_bias=qkv_bias)


EPSILON = 1e-06
THETA = 1000000.0
MASKED = -1e+30

def rms_norm(rows, gain):
    values = rows.astype(jnp.float32)
    return (values * lax.rsqrt(lax.optimization_barrier(jnp.mean(values * values, axis=-1, keepdims=True)) + EPSILON) * gain).astype(jnp.bfloat16)

def rotate(values, positions):
    head_size = values.shape[-1]
    half = head_size // 2
    steps = jnp.arange(half, dtype=jnp.float32) * (2.0 / head_size)
    frequency = jnp.exp(-math.log(THETA) * steps)
    angle = positions.astype(jnp.float32)[:, None] * frequency[None, :]
    cosine = jnp.cos(angle)[:, None, None, :]
    sine = jnp.sin(angle)[:, None, None, :]
    first = values[..., :half]
    second = values[..., half:]
    return jnp.concatenate([first * cosine - second * sine, second * cosine + first * sine], axis=-1)

def vision_heads(normed, weight, bias, windows, count, head_size):
    slot_count = normed.shape[0]
    mixed = jnp.dot(normed, weight, preferred_element_type=jnp.float32) + bias
    heads = mixed.shape[1] // (3 * head_size)
    mixed = mixed.astype(jnp.bfloat16).reshape(slot_count, heads, 3, head_size)
    query = mixed[:, :, 0].astype(jnp.float32)
    key = mixed[:, :, 1].astype(jnp.float32)
    value = mixed[:, :, 2].astype(jnp.float32)
    scores = jnp.einsum('rhd,shd->hrs', query, key) * (1.0 / math.sqrt(head_size))
    index = jnp.arange(slot_count, dtype=jnp.int32)
    allowed = (windows[:, None] == windows[None, :]) & ((index[None, :] < count) | (index[:, None] == index[None, :]))
    scores = jnp.where(allowed[None], scores, MASKED)
    top = lax.optimization_barrier(jnp.max(scores, axis=-1, keepdims=True))
    weights = jnp.where(allowed[None], jnp.exp(scores - top), 0.0)
    total = lax.optimization_barrier(jnp.sum(weights, axis=-1))
    result = jnp.einsum('hrs,shd->rhd', weights.astype(jnp.bfloat16).astype(jnp.float32), value)
    return (result / jnp.transpose(total)[:, :, None]).astype(jnp.bfloat16).reshape(slot_count, heads * head_size)

def causal_group(inputs):
    query, key, value = inputs
    scale = 1.0 / math.sqrt(HD)
    key_wide = key.astype(jnp.float32)
    value_wide = value.astype(jnp.float32)
    blocks = query.reshape(TOKENS // TOK_DEV, TOK_DEV, QH, HD)
    starts = jnp.arange(TOKENS // TOK_DEV, dtype=jnp.int32) * TOK_DEV
    key_pos = jnp.arange(TOKENS, dtype=jnp.int32)

    def one_block(block_inputs):
        block, first = block_inputs
        scores = jnp.einsum('rjd,sd->jrs', block.astype(jnp.float32), key_wide) * scale
        query_pos = first + jnp.arange(TOK_DEV, dtype=jnp.int32)
        allowed = key_pos[None, :] <= query_pos[:, None]
        scores = jnp.where(allowed[None], scores, MASKED)
        top = lax.optimization_barrier(jnp.max(scores, axis=-1, keepdims=True))
        weights = jnp.where(allowed[None], jnp.exp(scores - top), 0.0)
        total = lax.optimization_barrier(jnp.sum(weights, axis=-1))
        result = jnp.einsum('jrs,sd->rjd', weights.astype(jnp.bfloat16).astype(jnp.float32), value_wide)
        return (result / jnp.transpose(total)[:, :, None]).astype(jnp.bfloat16)
    return lax.map(one_block, (blocks, starts)).reshape(TOKENS, QH, HD)

def reference(patches, patch_count, token_patch, window_ids, text_embed, vit_norm_gain, vit_qkv, vit_qkv_bias, vit_proj, vit_proj_bias, merge_norm_gain, merger, merger_bias, llm_norm_gain, w_qkv, qkv_bias):
    normed = rms_norm(patches, vit_norm_gain)
    shard_rows = normed.reshape(N_CTX, TOK_DEV, DV)
    shard_windows = window_ids.reshape(N_CTX, TOK_DEV)

    def one_shard(inputs):
        rows, window_rows, count = inputs
        return vision_heads(rows, vit_qkv, vit_qkv_bias, window_rows, count, VHD)
    attended = lax.map(one_shard, (shard_rows, shard_windows, patch_count)).reshape(TOKENS, DV)
    vit_out = patches.astype(jnp.float32) + jnp.dot(attended, vit_proj, preferred_element_type=jnp.float32) + vit_proj_bias
    merged_in = rms_norm(vit_out, merge_norm_gain)
    image = (jnp.dot(merged_in, merger, preferred_element_type=jnp.float32) + merger_bias).astype(jnp.bfloat16)
    offsets = jnp.arange(TOKENS, dtype=jnp.int32) // TOK_DEV * TOK_DEV
    picked = jnp.take(image, offsets + jnp.maximum(token_patch, 0).astype(jnp.int32), axis=0)
    stitched = jnp.where(token_patch[:, None] >= 0, picked, text_embed)
    values = stitched.astype(jnp.float32)
    llm_in = (values * lax.rsqrt(lax.optimization_barrier(jnp.mean(values * values, axis=-1, keepdims=True)) + EPSILON) * llm_norm_gain).astype(jnp.bfloat16)
    projected = jnp.dot(llm_in, w_qkv, preferred_element_type=jnp.float32) + qkv_bias
    projected = projected.reshape(TOKENS, KVH, QH + 2, HD)
    positions = jnp.arange(TOKENS, dtype=jnp.int32)
    turned = rotate(projected[:, :, :QH + 1], positions).astype(jnp.bfloat16)
    queries = jnp.transpose(turned[:, :, :QH], (1, 0, 2, 3))
    keys_all = jnp.transpose(turned[:, :, QH], (1, 0, 2))
    values_all = jnp.transpose(projected[:, :, QH + 1].astype(jnp.bfloat16), (1, 0, 2))
    context = lax.map(causal_group, (queries, keys_all, values_all))
    return jnp.transpose(context, (1, 0, 2, 3)).reshape(TOKENS, KVH * QH * HD)
```

```python
import functools
import math

import jax
import jax.numpy as jnp
from jax import lax
from jax.experimental import pallas as pl
from jax.experimental.pallas import tpu as pltpu
from jax.sharding import PartitionSpec as P

VHD = 80
HD = 128
QH = 4
EPSILON = 1e-06
THETA = 1000000.0
MASKED = -1e30

PAIR, DEEP, WIDE = 2, 8, 4
ROWS, CORES = 4, 2
F32 = jnp.float32
BF16 = jnp.bfloat16


def ring_steps(n):
    return n // 2, (n - 1) // 2


def iota(shape, dim):
    return lax.broadcasted_iota(jnp.int32, shape, dim)


class Place:
    def __init__(self):
        ctx = lax.axis_index("ctx")
        head = lax.axis_index("head")
        self.ctx, self.head = ctx, head
        self.pair = ctx // (DEEP * WIDE)
        self.deep = (ctx // WIDE) % DEEP
        self.wide = ctx % WIDE
        self.row = head // CORES
        self.core = head % CORES
        self.sign = 1 - 2 * self.core

    def at_ctx(self, pair, deep, wide):
        return ((pair * DEEP + deep) * WIDE + wide, self.head)

    def at_head(self, row, core):
        return (self.ctx, row * CORES + core)

    def other_pair(self):
        return self.at_ctx(1 - self.pair, self.deep, self.wide)

    def deep_at(self, step):
        return (self.deep + step + 2 * DEEP) % DEEP

    def wide_at(self, step):
        return (self.wide + step + 2 * WIDE) % WIDE

    def neighbours(self):
        found = [self.other_pair()]
        found += [self.at_ctx(self.pair, self.deep_at(s), self.wide) for s in ((1, -1) if DEEP > 2 else (1,))]
        found += [self.at_ctx(self.pair, self.deep, self.wide_at(s)) for s in ((1, -1) if WIDE > 2 else (1,))]
        found += [self.at_head((self.row + k) % ROWS, self.core) for k in range(1, ROWS)]
        found.append(self.at_head(self.row, 1 - self.core))
        return found


class Copies:
    def __init__(self, send_sems, recv_sems):
        self.send_sems, self.recv_sems = send_sems, recv_sems
        self.used = 0
        self.sent = []

    def take(self):
        self.used += 1
        return self.used - 1

    def send(self, ref, slot, device):
        copy = pltpu.make_async_remote_copy(
            src_ref=ref,
            dst_ref=ref,
            send_sem=self.send_sems.at[slot],
            recv_sem=self.recv_sems.at[slot],
            device_id=device,
            device_id_type=pl.DeviceIdType.MESH,
        )
        copy.start()
        self.sent.append(copy)

    def wait(self, ref, slot, device):
        pltpu.make_async_remote_copy(
            src_ref=ref,
            dst_ref=ref,
            send_sem=self.send_sems.at[slot],
            recv_sem=self.recv_sems.at[slot],
            device_id=device,
            device_id_type=pl.DeviceIdType.MESH,
        ).wait_recv()

    def drain(self):
        for copy in self.sent:
            copy.wait_send()


class Chain:
    def __init__(self, copies, place, bundle, along_deep):
        self.copies, self.place, self.bundle = copies, place, bundle
        self.n = DEEP if along_deep else WIDE
        self.along_deep = along_deep
        self.steps = ring_steps(self.n)
        self.slots = [
            [[copies.take() for _ in range(PAIR)] for _ in range(count)] for count in self.steps
        ]

    def index(self, step):
        return self.place.deep_at(step) if self.along_deep else self.place.wide_at(step)

    def device(self, step):
        p = self.place
        if self.along_deep:
            return p.at_ctx(p.pair, p.deep_at(step), p.wide)
        return p.at_ctx(p.pair, p.deep, p.wide_at(step))

    def send(self, way, k, j):
        if k >= self.steps[way]:
            return
        sign = self.place.sign * (1 if way == 0 else -1)
        pair = self.place.pair if j == 0 else 1 - self.place.pair
        self.copies.send(self.bundle(pair, self.index(-sign * k)), self.slots[way][k][j], self.device(sign))

    def start(self, j):
        for way in range(2):
            self.send(way, 0, j)

    def tick(self, k):
        for j in range(PAIR):
            for way in range(2):
                if k < self.steps[way]:
                    sign = self.place.sign * (1 if way == 0 else -1)
                    pair = self.place.pair if j == 0 else 1 - self.place.pair
                    self.copies.wait(
                        self.bundle(pair, self.index(-sign * (k + 1))), self.slots[way][k][j], self.device(sign)
                    )
                    self.send(way, k + 1, j)


class CtxGather:
    def __init__(self, copies, place, buf, first, second):
        self.copies, self.place, self.buf = copies, place, buf
        p = place
        self.swap = copies.take()
        self.first_wide = Chain(copies, p, lambda j, i: buf.at[(j, p.deep, i) + first], False)
        self.first_deep = Chain(copies, p, lambda j, i: buf.at[(j, i, slice(None)) + first], True)
        self.second_deep = Chain(copies, p, lambda j, i: buf.at[(j, i, p.wide) + second], True)
        self.second_wide = Chain(copies, p, lambda j, i: buf.at[(j, slice(None), i) + second], False)
        self.ticks = 0
        w, d = WIDE // 2, DEEP // 2
        self.last = max(w + d, d + w)

    def start(self):
        p = self.place
        self.copies.send(self.buf.at[p.pair, p.deep, p.wide], self.swap, p.other_pair())
        self.first_wide.start(0)
        self.second_deep.start(0)

    def swapped(self):
        p = self.place
        self.copies.wait(self.buf.at[1 - p.pair, p.deep, p.wide], self.swap, p.other_pair())
        self.first_wide.start(1)
        self.second_deep.start(1)

    def tick(self):
        t = self.ticks
        w, d = WIDE // 2, DEEP // 2
        if t < w:
            self.first_wide.tick(t)
            if t == w - 1:
                self.first_deep.start(0)
                self.first_deep.start(1)
        elif t < w + d:
            self.first_deep.tick(t - w)
        if t < d:
            self.second_deep.tick(t)
            if t == d - 1:
                self.second_wide.start(0)
                self.second_wide.start(1)
        elif t < w + d:
            self.second_wide.tick(t - d)
        self.ticks += 1

    def done(self):
        return self.ticks >= WIDE // 2 + DEEP // 2


class HeadGather:
    def __init__(self, copies, place, buf):
        self.copies, self.place, self.buf = copies, place, buf
        self.own = [copies.take() for _ in range(ROWS)]
        self.passed = [copies.take() for _ in range(1, ROWS)]

    def slot(self, back, core):
        return ((self.place.row - back + ROWS) % ROWS) * CORES + core

    def start(self):
        p = self.place
        mine = self.buf.at[p.head]
        for k in range(1, ROWS):
            self.copies.send(mine, self.own[k], p.at_head((p.row + k) % ROWS, p.core))
        self.copies.send(mine, self.own[0], p.at_head(p.row, 1 - p.core))

    def order(self):
        return [k for k in range(1, ROWS) if k != 2] + ([2] if ROWS > 2 else [])

    def pass_on(self):
        p = self.place
        for k in self.order():
            ref = self.buf.at[self.slot(k, p.core)]
            self.copies.wait(ref, self.own[k], p.at_head(p.row, 1 - p.core))
            self.copies.send(ref, self.passed[k - 1], p.at_head(p.row, 1 - p.core))

    def finish(self):
        p = self.place
        other = p.at_head(p.row, 1 - p.core)
        self.copies.wait(self.buf.at[self.slot(0, 1 - p.core)], self.own[0], other)
        for k in self.order():
            self.copies.wait(self.buf.at[self.slot(k, 1 - p.core)], self.passed[k - 1], other)


def dot(a, b):
    return jnp.dot(a, b, preferred_element_type=F32)


def dot_nt(a, b):
    return lax.dot_general(a, b, (((1,), (1,)), ((), ())), preferred_element_type=F32)


def across(row, size):
    return jnp.transpose(jnp.broadcast_to(row, (size, row.shape[1])))


def vision(patches, gain, weight, bias, windows, count):
    tok = patches.shape[0]
    values = patches.astype(F32)
    normed = values * lax.rsqrt(jnp.mean(values * values, axis=-1, keepdims=True) + EPSILON) * gain
    mixed = (dot(normed.astype(BF16), weight) + bias).astype(BF16)
    width = mixed.shape[1]
    parts = width // VHD
    heads = parts // 3
    row, col = iota((width, parts * 128), 0), iota((width, parts * 128), 1)
    lane = col & 127
    spread = jnp.where((row == (col >> 7) * VHD + lane) & (lane < VHD), 1.0, 0.0).astype(BF16)
    wide = dot(mixed, spread).astype(BF16)
    down = across(windows, tok)
    row, col = iota((tok, tok), 0), iota((tok, tok), 1)
    allowed = (down == windows) & ((col < count) | (row == col))
    results = []
    for h in range(heads):
        query, key, value = (wide[:, (3 * h + i) * 128 : (3 * h + i + 1) * 128] for i in range(3))
        scores = jnp.where(allowed, dot_nt(query, key) * (1.0 / math.sqrt(VHD)), MASKED)
        top = jnp.max(scores, axis=-1, keepdims=True)
        weights = jnp.where(allowed, jnp.exp(scores - top), 0.0)
        total = jnp.sum(weights, axis=-1, keepdims=True)
        results.append((dot(weights.astype(BF16), value) / total).astype(BF16))
    both = jnp.concatenate(results, axis=1)
    row, col = iota((heads * 128, heads * VHD), 0), iota((heads * 128, heads * VHD), 1)
    lane = row & 127
    pack = jnp.where((col == (row >> 7) * VHD + lane) & (lane < VHD), 1.0, 0.0).astype(BF16)
    return dot(both, pack).astype(BF16)


def widen(merged, blocks):
    share = merged.shape[1] // (PAIR * DEEP * WIDE)
    span = blocks * share
    row, col = iota((span, blocks * 32), 0), iota((span, blocks * 32), 1)
    main = col < blocks * 16
    near = jnp.where(main, col, col - blocks * 16)
    block, place = near >> 4, near & 15
    want = block * share + jnp.where(main, place, 16 + (place & 3))
    spread = jnp.where(row == want, 1.0, 0.0).astype(BF16)
    return [
        dot(merged[:, at * span : (at + 1) * span], spread).astype(BF16)
        for at in range(merged.shape[1] // span)
    ]


def turn(x, cosine, sine):
    return x * cosine + pltpu.roll(x, HD // 2, 1) * sine


def attend(state, query, keys, values, allowed):
    scores = dot_nt(query, keys) * (1.0 / math.sqrt(HD))
    if allowed is not None:
        scores = jnp.where(allowed, scores, MASKED)
    here = jnp.max(scores, axis=-1, keepdims=True)
    if state is None:
        top = here
    else:
        top = jnp.maximum(state[0], here)
    weights = jnp.exp(scores - top)
    if allowed is not None:
        weights = jnp.where(allowed, weights, 0.0)
    total = jnp.sum(weights, axis=-1, keepdims=True)
    result = dot(weights.astype(BF16), values)
    if state is not None:
        factor = jnp.exp(state[0] - top)
        total = state[1] * factor + total
        result = state[2] * factor + result
    return top, total, result


def kernel(
    patches,
    count,
    token_patch,
    windows,
    text,
    vit_gain,
    vit_qkv,
    vit_bias,
    vit_proj,
    proj_bias,
    merge_gain,
    merger,
    merger_bias,
    llm_gain,
    w_qkv,
    qkv_bias,
    out,
    merge_buf,
    weight_buf,
    proj_buf,
    att_buf,
    stitch_buf,
    kv_buf,
    query_buf,
    local_sems,
    send_sems,
    recv_sems,
):
    place = Place()
    p = place
    barrier = pltpu.get_barrier_semaphore()
    around = p.neighbours()
    for device in around:
        pl.semaphore_signal(barrier, inc=1, device_id=device, device_id_type=pl.DeviceIdType.MESH)
    local = [
        pltpu.make_async_copy(merger, merge_buf.at[p.pair, p.deep, p.wide], local_sems.at[0]),
        pltpu.make_async_copy(w_qkv, weight_buf.at[p.pair, p.deep, p.wide], local_sems.at[1]),
        pltpu.make_async_copy(vit_proj, proj_buf.at[p.head], local_sems.at[2]),
    ]
    for copy in local:
        copy.start()
    for copy in local:
        copy.wait()
    pl.semaphore_wait(barrier, len(around))

    tok, features = patches.shape
    width = text.shape[1]
    columns = w_qkv.shape[1]
    every = slice(None)
    copies = Copies(send_sems, recv_sems)
    cut = (merger.shape[1] // 256) * 128
    merge_gather = CtxGather(copies, p, merge_buf, (every, slice(0, cut)), (every, slice(cut, None)))
    cut = (columns // 256) * 128
    weight_gather = CtxGather(copies, p, weight_buf, (every, slice(0, cut)), (every, slice(cut, None)))
    cut = tok // 2
    kv_gather = CtxGather(copies, p, kv_buf, (slice(0, cut), every), (slice(cut, None), every))
    proj_gather = HeadGather(copies, p, proj_buf)
    att_gather = HeadGather(copies, p, att_buf)
    stitch_gather = HeadGather(copies, p, stitch_buf)

    merge_gather.start()
    weight_gather.start()
    proj_gather.start()

    att_buf[p.head] = vision(
        patches[...], vit_gain[...], vit_qkv[...], vit_bias[...], windows[...], count[...]
    )
    merge_gather.swapped()
    weight_gather.swapped()
    att_gather.start()
    while not merge_gather.done():
        merge_gather.tick()
        if merge_gather.ticks % 2 == 0 and weight_gather.ticks < 2:
            weight_gather.tick()
    att_gather.pass_on()
    proj_gather.pass_on()
    weight_gather.tick()
    att_gather.finish()
    proj_gather.finish()

    vit_out = patches[...].astype(F32) + proj_bias[...]
    for h in range(ROWS * CORES):
        vit_out += dot(att_buf[h], proj_buf[h])
    merged = vit_out * lax.rsqrt(jnp.mean(vit_out * vit_out, axis=-1, keepdims=True) + EPSILON)
    merged = (merged * merge_gain[...]).astype(BF16)
    blocks = DEEP * WIDE
    spreads = widen(merged, blocks)
    image = jnp.broadcast_to(merger_bias[...], (tok, width))
    tails = [jnp.zeros((tok, 128), F32) for _ in range(4)]
    for g in range(PAIR):
        rows = merge_buf[g].reshape(blocks * 16, merger.shape[1])
        image += dot(spreads[g][:, : blocks * 16], rows[:, :width])
        rest = spreads[g][:, blocks * 16 :]
        lane = iota(rest.shape, 1)
        for j in range(4):
            chosen = jnp.where(((lane >> 2) & 3) == j, rest.astype(F32), 0.0).astype(BF16)
            tails[j] += dot(chosen, rows[:, width:])
    image = (image + jnp.concatenate(tails, axis=1)).astype(BF16)
    down = across(token_patch[...], tok)
    chosen = jnp.where(down == iota((tok, tok), 1), 1.0, 0.0).astype(BF16)
    picked = dot(chosen, image)
    stitch_buf[p.head] = jnp.where(down[:, :1] >= 0, picked, text[...].astype(F32)).astype(BF16)
    stitch_gather.start()

    lane = iota((tok, HD), 1)
    step = (lane & (HD // 2 - 1)).astype(F32) * (2.0 / HD)
    angle = (p.ctx * tok + iota((tok, HD), 0)).astype(F32) * jnp.exp(-math.log(THETA) * step)
    cosine = jnp.cos(angle)
    sine = jnp.where(lane < HD // 2, -1.0, 1.0) * jnp.sin(angle)

    weight_gather.tick()
    stitch_gather.pass_on()
    weight_gather.tick()
    stitch_gather.finish()
    while not weight_gather.done():
        weight_gather.tick()

    square = jnp.zeros((tok, width), F32)
    for h in range(ROWS * CORES):
        block = stitch_buf[h].astype(F32)
        square += block * block
    scale = lax.rsqrt(jnp.sum(square, axis=-1, keepdims=True) / (ROWS * CORES * width) + EPSILON)
    projected = jnp.broadcast_to(qkv_bias[...], (tok, columns))
    span = width // w_qkv.shape[0]
    for h in range(ROWS * CORES):
        block = (stitch_buf[h].astype(F32) * scale * llm_gain[:, h * width : (h + 1) * width]).astype(BF16)
        first = h * span
        if span >= WIDE:
            rows = weight_buf[first // (DEEP * WIDE), pl.ds((first // WIDE) % DEEP, span // WIDE)]
        else:
            rows = weight_buf[first // (DEEP * WIDE), (first // WIDE) % DEEP, pl.ds(first % WIDE, span)]
        projected += dot(block, rows.reshape(width, columns))
    key = turn(projected[:, QH * HD : (QH + 1) * HD], cosine, sine).astype(BF16)
    kv_buf[p.pair, p.deep, p.wide, :, :HD] = key
    kv_buf[p.pair, p.deep, p.wide, :, HD:] = projected[:, (QH + 1) * HD :].astype(BF16)
    for j in range(QH):
        query_buf[j * tok : (j + 1) * tok] = turn(
            projected[:, j * HD : (j + 1) * HD], cosine, sine
        ).astype(BF16)
    kv_gather.start()
    kv_gather.swapped()
    while not kv_gather.done():
        kv_gather.tick()

    query = query_buf[...]
    group = p.pair * DEEP + p.deep
    keys = WIDE * tok
    rows, cols = iota((QH * tok, keys), 0), iota((QH * tok, keys), 1)
    allowed = cols <= p.wide * tok + (rows & (tok - 1))
    own = kv_buf[p.pair, p.deep].reshape(keys, 2 * HD)
    state = attend(None, query, own[:, :HD], own[:, HD:], allowed)

    def visit(unit, state):
        block = kv_buf[unit // DEEP, unit % DEEP].reshape(keys, 2 * HD)
        return attend(state, query, block[:, :HD], block[:, HD:], None)

    _, total, result = lax.fori_loop(0, group, visit, state)
    result = (result / total).astype(BF16)
    for j in range(QH):
        out[:, j * HD : (j + 1) * HD] = result[j * tok : (j + 1) * tok]
    copies.drain()


def body(
    patches,
    patch_count,
    token_patch,
    window_ids,
    text_embed,
    vit_norm_gain,
    vit_qkv,
    vit_qkv_bias,
    vit_proj,
    vit_proj_bias,
    merge_norm_gain,
    merger,
    merger_bias,
    llm_norm_gain,
    w_qkv,
    qkv_bias,
):
    tok, features = patches.shape
    share, width = merger.shape
    rest = merger[16:].reshape(4, width // 128, 128)
    rest = jnp.transpose(rest, (1, 0, 2)).reshape(16, 128)
    merger_tile = jnp.concatenate([merger[:16], rest], axis=1)
    line = lambda vector: vector.reshape(1, -1)
    vmem = pl.BlockSpec(memory_space=pltpu.VMEM)
    hbm = pl.BlockSpec(memory_space=pltpu.HBM)
    specs = [vmem] * 16
    specs[8] = specs[11] = specs[14] = hbm
    ctx_shape = (PAIR, DEEP, WIDE)
    heads = ROWS * CORES
    per_ctx = 1 + 2 * (WIDE - 1 + DEEP - 1) * PAIR
    slots = 3 * per_ctx + 3 * (2 * ROWS - 1)
    return pl.pallas_call(
        kernel,
        out_shape=jax.ShapeDtypeStruct((tok, QH * HD), BF16),
        in_specs=specs,
        out_specs=vmem,
        scratch_shapes=[
            pltpu.VMEM(ctx_shape + merger_tile.shape, BF16),
            pltpu.VMEM(ctx_shape + w_qkv.shape, BF16),
            pltpu.VMEM((heads,) + vit_proj.shape, BF16),
            pltpu.VMEM((heads, tok, vit_proj.shape[0]), BF16),
            pltpu.VMEM((heads,) + text_embed.shape, BF16),
            pltpu.VMEM(ctx_shape + (tok, 2 * HD), BF16),
            pltpu.VMEM((QH * tok, HD), BF16),
            pltpu.SemaphoreType.DMA((3,)),
            pltpu.SemaphoreType.DMA((slots,)),
            pltpu.SemaphoreType.DMA((slots,)),
        ],
        compiler_params=pltpu.CompilerParams(
            collective_id=0, has_side_effects=True, vmem_limit_bytes=60 * 1024 * 1024
        ),
        name="whole",
    )(
        patches,
        patch_count.reshape(1, 1),
        line(token_patch),
        line(window_ids),
        text_embed,
        line(vit_norm_gain),
        vit_qkv,
        line(vit_qkv_bias),
        vit_proj,
        line(vit_proj_bias),
        line(merge_norm_gain),
        merger_tile,
        line(merger_bias),
        line(llm_norm_gain),
        w_qkv,
        line(qkv_bias),
    )


def solution(mesh):
    return jax.shard_map(
        body,
        mesh=mesh,
        in_specs=(
            P("ctx", None),
            P("ctx"),
            P("ctx"),
            P("ctx"),
            P("ctx", "head"),
            P(),
            P(None, "head"),
            P("head"),
            P("head", None),
            P(),
            P(),
            P("ctx", "head"),
            P("head"),
            P(),
            P("ctx", "head"),
            P("head"),
        ),
        out_specs=P("ctx", "head"),
        check_vma=False,
    )
```

```python
import functools
import math

import jax
import jax.numpy as jnp
from jax import lax
from jax.experimental import pallas as pl
from jax.experimental.pallas import tpu as pltpu
from jax.sharding import PartitionSpec as P

VHD = 80
HD = 128
QH = 4
EPSILON = 1e-06
THETA = 1000000.0
MASKED = -1e30

PAIR, DEEP, WIDE = 2, 8, 4
ROWS, CORES = 4, 2
F32 = jnp.float32
BF16 = jnp.bfloat16


def iota(shape, dim):
    return lax.broadcasted_iota(jnp.int32, shape, dim)


class Place:
    def __init__(self):
        ctx = lax.axis_index("ctx")
        head = lax.axis_index("head")
        self.ctx, self.head = ctx, head
        self.pair = ctx // (DEEP * WIDE)
        self.deep = (ctx // WIDE) % DEEP
        self.wide = ctx % WIDE
        self.row = head // CORES
        self.core = head % CORES
        self.high = self.row * PAIR + self.pair
        self.sign = 1 - 2 * self.core
        self.side = 2 * self.pair - 1

    def at_ctx(self, pair, deep, wide):
        return ((pair * DEEP + deep) * WIDE + wide, self.head)

    def at_head(self, row, core):
        return (self.ctx, row * CORES + core)

    def at_high(self, step):
        high = self.high_at(step)
        ctx = ((high % PAIR) * DEEP + self.deep) * WIDE + self.wide
        return (ctx, (high // PAIR) * CORES + self.core)

    def high_at(self, step):
        return (self.high + step + 2 * ROWS * PAIR) % (ROWS * PAIR)

    def other_core(self):
        return self.at_head(self.row, 1 - self.core)

    def other_pair(self):
        return self.at_ctx(1 - self.pair, self.deep, self.wide)

    def next_pair(self):
        return self.at_high(self.side)

    def deep_at(self, step):
        return (self.deep + step + 2 * DEEP) % DEEP

    def wide_at(self, step):
        return (self.wide + step + 2 * WIDE) % WIDE

    def at_deep(self, step):
        return self.at_ctx(self.pair, self.deep_at(step), self.wide)

    def at_wide(self, step):
        return self.at_ctx(self.pair, self.deep, self.wide_at(step))

    def neighbours(self):
        found = [self.other_pair(), self.next_pair(), self.at_deep(1), self.at_deep(-1)]
        found += [self.at_wide(k) for k in range(1, WIDE)]
        found += [self.at_head((self.row + k) % ROWS, self.core) for k in range(1, ROWS)]
        found.append(self.other_core())
        return found


class Copies:
    def __init__(self, send_sems, recv_sems):
        self.send_sems, self.recv_sems = send_sems, recv_sems
        self.used = 0
        self.sent = []

    def take(self, count):
        self.used += count
        return list(range(self.used - count, self.used))

    def copy(self, source, target, slot, device):
        return pltpu.make_async_remote_copy(
            src_ref=source,
            dst_ref=target,
            send_sem=self.send_sems.at[slot],
            recv_sem=self.recv_sems.at[slot],
            device_id=device,
            device_id_type=pl.DeviceIdType.MESH,
        )

    def send(self, make, slot, device, target=None, some=False):
        self.copy(make(), (target or make)(), slot, device()).start()
        self.sent.append((make, target or make, slot, device, some))

    def wait(self, ref, slot, device):
        self.copy(ref, ref, slot, device).wait_recv()

    def drain(self, some):
        for make, target, slot, device, kind in self.sent:
            if kind == some:
                self.copy(make(), target(), slot, device()).wait_send()


class PlaneGather:
    def __init__(self, copies, place, buf, rows, some=(False, False)):
        self.copies, self.place, self.buf, self.some = copies, place, buf, some
        self.first, self.second = slice(0, rows), slice(rows, None)
        self.early = [copies.take(WIDE - 1) for _ in range(2)]
        self.bundles = [copies.take(DEEP) for _ in range(2)]
        self.singles = [copies.take(DEEP) for _ in range(2)]
        self.across = [[copies.take(WIDE - 1) for _ in range(DEEP)] for _ in range(2)]

    def offset(self, t):
        return self.place.sign * ((t + 1) // 2) * (-1 if t % 2 else 1)

    def way(self, t):
        return self.place.sign * (1 if t % 2 else -1)

    def bundle(self, pair, t):
        return self.buf.at[pair, self.place.deep_at(self.offset(t)), :, self.first]

    def single(self, pair, t, step=0):
        p = self.place
        return self.buf.at[pair, p.deep_at(self.offset(t)), p.wide_at(step), self.second]

    def along(self, slots, make, j, t):
        p = self.place
        for later in (1, 2) if t == 0 else (t + 2,):
            if later < DEEP:
                self.copies.send(
                    make, slots[j][later], lambda later=later: p.at_deep(self.way(later)), some=self.some[j]
                )

    def sideways(self, pair, j, t):
        p = self.place
        for k, step in ((0, 1), (1, -1)):
            self.copies.send(
                lambda: self.single(pair, t),
                self.across[j][t][k],
                lambda step=step: p.at_wide(p.sign * step),
                some=self.some[j],
            )

    def start(self, pair, j):
        p = self.place
        self.along(self.singles, lambda: self.single(pair, 0), j, 0)
        for k in range(1, WIDE):
            self.copies.send(
                lambda: self.buf.at[pair, p.deep, p.wide, self.first],
                self.early[j][k - 1],
                lambda k=k: p.at_wide(k),
                some=self.some[j],
            )
        self.sideways(pair, j, 0)

    def arrive(self, pair, j, t):
        p = self.place
        if t == 0:
            for k in range(1, WIDE):
                ref = self.buf.at[pair, p.deep, p.wide_at(-k), self.first]
                self.copies.wait(ref, self.early[j][k - 1], p.other_core())
            self.along(self.bundles, lambda: self.bundle(pair, 0), j, 0)
        else:
            self.copies.wait(self.single(pair, t), self.singles[j][t], p.other_core())
            self.along(self.singles, lambda: self.single(pair, t), j, t)
            self.sideways(pair, j, t)
            self.copies.wait(self.bundle(pair, t), self.bundles[j][t], p.other_core())
            self.along(self.bundles, lambda: self.bundle(pair, t), j, t)

    def pass_on(self, pair, j, t):
        p = self.place
        self.copies.wait(self.single(pair, t, -p.sign), self.across[j][t][0], p.other_core())
        self.copies.send(
            lambda: self.single(pair, t, -p.sign),
            self.across[j][t][2],
            lambda: p.at_wide(p.sign),
            some=self.some[j],
        )

    def finish(self, pair, j, t):
        p = self.place
        self.copies.wait(self.single(pair, t, p.sign), self.across[j][t][1], p.other_core())
        self.copies.wait(self.single(pair, t, -2 * p.sign), self.across[j][t][2], p.other_core())

    def step(self, pair, j, t):
        if t < DEEP:
            self.arrive(pair, j, t)
        if 0 <= t - 1 < DEEP:
            self.pass_on(pair, j, t - 1)
        if 0 <= t - 2 < DEEP:
            self.finish(pair, j, t - 2)


class HeadGather:
    def __init__(self, copies, place, buf):
        self.copies, self.place, self.buf = copies, place, buf
        self.own = copies.take(ROWS)
        self.passed = copies.take(ROWS)

    def block(self, back, core):
        return self.buf.at[((self.place.row - back + ROWS) % ROWS) * CORES + core]

    def start(self):
        p = self.place
        for k in range(1, ROWS):
            self.copies.send(
                lambda: self.buf.at[p.head],
                self.own[k],
                lambda k=k: p.at_head((p.row + k) % ROWS, p.core),
            )
        self.copies.send(lambda: self.buf.at[p.head], self.own[0], p.other_core)

    def pass_on(self):
        p = self.place
        for k in (1, 3, 2):
            self.copies.wait(self.block(k, p.core), self.own[k], p.other_core())
            self.copies.send(lambda k=k: self.block(k, p.core), self.passed[k], p.other_core)

    def finish(self):
        p = self.place
        self.copies.wait(self.block(0, 1 - p.core), self.own[0], p.other_core())
        for k in (1, 3, 2):
            self.copies.wait(self.block(k, 1 - p.core), self.passed[k], p.other_core())


class ProjGather:
    def __init__(self, copies, place, buf):
        self.copies, self.place, self.buf = copies, place, buf
        self.slots = copies.take(6)
        self.passed = copies.take(7)

    def half(self, step, core, half):
        rows = self.buf.shape[1] // 2
        row = (self.place.row + step + ROWS) % ROWS
        return self.buf.at[row * CORES + core, pl.ds(pl.multiple_of(half * rows, 16), rows)]

    def piece(self, event, core):
        p = self.place
        step = (p.side, p.side, -p.side, -p.side, 2, 2)[event]
        half = (p.pair, 1 - p.pair, 1 - p.pair, p.pair, p.pair, 1 - p.pair)[event]
        return self.half(step, core, half)

    def start(self):
        p = self.place
        for event, half in ((0, 1 - p.pair), (1, p.pair)):
            self.copies.send(lambda half=half: self.half(0, p.core, half), self.slots[event], p.next_pair)
        self.copies.send(lambda: self.buf.at[p.head], self.passed[6], p.other_core)

    def event(self, event):
        p = self.place
        make = lambda: self.piece(event, p.core)
        self.copies.wait(make(), self.slots[event], p.other_core())
        if event in (0, 1):
            self.copies.send(make, self.slots[event + 2], p.other_pair)
        if event == 2:
            self.copies.send(make, self.slots[4], p.next_pair)
        if event == 4:
            self.copies.send(make, self.slots[5], p.other_pair)
        self.copies.send(make, self.passed[event], p.other_core)

    def finish(self):
        p = self.place
        other = 1 - p.core
        self.copies.wait(self.buf.at[p.row * CORES + other], self.passed[6], p.other_core())
        for event in range(6):
            self.copies.wait(self.piece(event, other), self.passed[event], p.other_core())


class RingGather:
    def __init__(self, copies, place, buf, pieces):
        self.copies, self.place, self.buf, self.pieces = copies, place, buf, pieces
        self.size = ROWS * PAIR
        self.slots = [copies.take(self.size) for _ in range(pieces)]
        self.passed = [copies.take(self.size) for _ in range(pieces)]

    def piece(self, t, core, i, sign):
        rows = self.buf.shape[2] // self.pieces
        offset = sign * ((t + 1) // 2) * (-1 if t % 2 else 1)
        return self.buf.at[self.place.high_at(offset), core, i * rows : (i + 1) * rows]

    def send(self, t, i):
        p = self.place
        make = lambda: self.piece(t, p.core, i, p.sign)
        for later in (1, 2) if t == 0 else (t + 2,):
            if later < self.size:
                step = p.sign * (1 if later % 2 else -1)
                self.copies.send(make, self.slots[i][later], lambda step=step: p.at_high(step))
        self.copies.send(make, self.passed[i][t], p.other_core)

    def start(self):
        for i in range(self.pieces):
            self.send(0, i)

    def step(self, t):
        p = self.place
        for i in range(self.pieces):
            self.copies.wait(self.piece(t, p.core, i, p.sign), self.slots[i][t], p.other_core())
            self.send(t, i)

    def finish(self):
        p = self.place
        for t in range(self.size):
            for i in range(self.pieces):
                self.copies.wait(self.piece(t, 1 - p.core, i, -p.sign), self.passed[i][t], p.other_core())


def dot(a, b):
    return jnp.dot(a, b, preferred_element_type=F32)


def dot_nt(a, b):
    return lax.dot_general(a, b, (((1,), (1,)), ((), ())), preferred_element_type=F32)


def across(row, size):
    return jnp.transpose(jnp.broadcast_to(row, (size, row.shape[1])))


def vision(patches, gain, weight, bias, windows, count):
    tok = patches.shape[0]
    values = patches.astype(F32)
    normed = values * lax.rsqrt(jnp.mean(values * values, axis=-1, keepdims=True) + EPSILON) * gain
    mixed = (dot_nt(normed.astype(BF16), weight) + bias).astype(BF16)
    width = mixed.shape[1]
    parts = width // VHD
    heads = parts // 3
    row, col = iota((width, parts * 128), 0), iota((width, parts * 128), 1)
    lane = col & 127
    spread = jnp.where((row == (col >> 7) * VHD + lane) & (lane < VHD), 1.0, 0.0).astype(BF16)
    wide = dot(mixed, spread).astype(BF16)
    down = across(windows, tok)
    row, col = iota((tok, tok), 0), iota((tok, tok), 1)
    allowed = (down == windows) & ((col < count) | (row == col))
    results = []
    for h in range(heads):
        query, key, value = (wide[:, (3 * h + i) * 128 : (3 * h + i + 1) * 128] for i in range(3))
        scores = jnp.where(allowed, dot_nt(query, key) * (1.0 / math.sqrt(VHD)), MASKED)
        top = jnp.max(scores, axis=-1, keepdims=True)
        weights = jnp.where(allowed, jnp.exp(scores - top), 0.0)
        total = jnp.sum(weights, axis=-1, keepdims=True)
        results.append((dot(weights.astype(BF16), value) / total).astype(BF16))
    both = jnp.concatenate(results, axis=1)
    row, col = iota((heads * 128, heads * VHD), 0), iota((heads * 128, heads * VHD), 1)
    lane = row & 127
    pack = jnp.where((col == (row >> 7) * VHD + lane) & (lane < VHD), 1.0, 0.0).astype(BF16)
    return dot(both, pack).astype(BF16)


def widen(merged, blocks):
    share = merged.shape[1] // (PAIR * DEEP * WIDE)
    span = blocks * share
    row, col = iota((span, blocks * 32), 0), iota((span, blocks * 32), 1)
    main = col < blocks * 16
    near = jnp.where(main, col, col - blocks * 16)
    block, place = near >> 4, near & 15
    want = block * share + jnp.where(main, place, 16 + (place & 3))
    spread = jnp.where(row == want, 1.0, 0.0).astype(BF16)
    return [
        dot(merged[:, at * span : (at + 1) * span], spread).astype(BF16)
        for at in range(merged.shape[1] // span)
    ]


def turn(x, cosine, sine):
    return x * cosine + pltpu.roll(x, HD // 2, 1) * sine


def attend(top_ref, total_ref, sum_ref, query_ref, block, allowed):
    keys = block.shape[0] * block.shape[1]
    block = block.reshape(keys, 2 * HD)
    scores = dot_nt(query_ref[...], block[:, :HD]) * (1.0 / math.sqrt(HD))
    if allowed is not None:
        scores = jnp.where(allowed, scores, MASKED)
    top = jnp.max(scores, axis=-1, keepdims=True)
    if allowed is None:
        old = top_ref[...]
        top = jnp.maximum(top, old)
        factor = jnp.exp(old - top)
    weights = jnp.exp(scores - top)
    if allowed is not None:
        weights = jnp.where(allowed, weights, 0.0)
    total = jnp.sum(weights, axis=-1, keepdims=True)
    result = dot(weights.astype(BF16), block[:, HD:])
    if allowed is None:
        total = total_ref[...] * factor + total
        result = sum_ref[...] * factor + result
    top_ref[...] = top
    total_ref[...] = total
    sum_ref[...] = result


def kernel(
    patches,
    count,
    token_patch,
    windows,
    text,
    vit_gain,
    vit_qkv,
    vit_bias,
    vit_proj,
    proj_bias,
    merge_gain,
    merger,
    merger_bias,
    llm_gain,
    w_qkv,
    qkv_bias,
    out,
    merge_buf,
    weight_buf,
    proj_buf,
    att_buf,
    stitch_buf,
    mine_buf,
    theirs_buf,
    kv_buf,
    query_buf,
    top_ref,
    total_ref,
    sum_ref,
    local_sems,
    send_sems,
    recv_sems,
):
    p = Place()
    barrier = pltpu.get_barrier_semaphore()
    around = p.neighbours()
    for device in around:
        pl.semaphore_signal(barrier, inc=1, device_id=device, device_id_type=pl.DeviceIdType.MESH)
    tok, features = patches.shape
    width = text.shape[1]
    columns = w_qkv.shape[1] // 2
    line = lambda ref: ref[...].reshape(1, -1)

    def half(pair):
        return w_qkv.at[:, pl.ds(pl.multiple_of(pair * columns, 128), columns)]

    local = [
        pltpu.make_async_copy(half(p.pair), weight_buf.at[p.pair, p.deep, p.wide], local_sems.at[0]),
        pltpu.make_async_copy(vit_proj, proj_buf.at[p.head], local_sems.at[1]),
    ]
    for copy in local:
        copy.start()
    rest = merger[16:].astype(F32)
    rest = jnp.concatenate([rest[:, j * 128 : (j + 1) * 128] for j in range(4)], axis=0)
    merge_buf[p.pair, p.deep, p.wide, :, :width] = merger[:16]
    merge_buf[p.pair, p.deep, p.wide, :, width:] = rest.astype(BF16)
    for copy in local:
        copy.wait()
    pl.semaphore_wait(barrier, len(around))

    copies = Copies(send_sems, recv_sems)
    swaps = copies.take(3)
    merge_gather = PlaneGather(copies, p, merge_buf, 8)
    weight_gather = PlaneGather(copies, p, weight_buf, w_qkv.shape[0] // 2)
    kv_gather = PlaneGather(copies, p, kv_buf, tok // 2, (False, True))
    proj_gather = ProjGather(copies, p, proj_buf)
    att_gather = HeadGather(copies, p, att_buf)
    stitch_gather = RingGather(copies, p, stitch_buf, 2)

    own = lambda buf: buf.at[p.pair, p.deep, p.wide]
    copies.send(lambda: own(merge_buf), swaps[0], p.other_pair)
    copies.send(lambda: half(1 - p.pair), swaps[1], p.other_pair, lambda: own(weight_buf))
    merge_gather.start(p.pair, 0)
    proj_gather.start()
    weight_gather.start(p.pair, 0)

    att_buf[p.head] = vision(
        patches[...], line(vit_gain), vit_qkv[...], line(vit_bias), line(windows), count[...]
    )
    for gather, buf, slot in ((merge_gather, merge_buf, 0), (weight_gather, weight_buf, 1)):
        copies.wait(buf.at[1 - p.pair, p.deep, p.wide], swaps[slot], p.other_pair())
        gather.start(1 - p.pair, 1)
    att_gather.start()

    def both(t):
        for gather in (merge_gather, weight_gather):
            gather.step(p.pair, 0, t)
            gather.step(1 - p.pair, 1, t)

    both(0)
    both(1)
    proj_gather.event(0)
    both(2)
    proj_gather.event(1)
    both(3)
    proj_gather.event(2)
    att_gather.pass_on()
    both(4)
    proj_gather.event(3)
    both(5)
    proj_gather.event(4)
    both(6)
    proj_gather.event(5)
    for t in range(7, DEEP + 2):
        merge_gather.step(p.pair, 0, t)
        merge_gather.step(1 - p.pair, 1, t)
    att_gather.finish()
    proj_gather.finish()

    vit_out = patches[...].astype(F32) + line(proj_bias)
    for h in range(ROWS * CORES):
        vit_out += dot(att_buf[h], proj_buf[h])
    merged = vit_out * lax.rsqrt(jnp.mean(vit_out * vit_out, axis=-1, keepdims=True) + EPSILON)
    merged = (merged * line(merge_gain)).astype(BF16)
    blocks = DEEP * WIDE
    spreads = widen(merged, blocks)
    image = jnp.broadcast_to(line(merger_bias), (tok, width))
    tails = [jnp.zeros((tok, 128), F32) for _ in range(4)]
    for g in range(PAIR):
        rows = merge_buf[g].reshape(blocks * 16, width + 128)
        image += dot(spreads[g][:, : blocks * 16], rows[:, :width])
        rest = spreads[g][:, blocks * 16 :]
        lane = iota(rest.shape, 1)
        for j in range(4):
            chosen = jnp.where(((lane >> 2) & 3) == j, rest.astype(F32), 0.0).astype(BF16)
            tails[j] += dot(chosen, rows[:, width:])
    image = (image + jnp.concatenate(tails, axis=1)).astype(BF16)
    down = across(line(token_patch), tok)
    chosen = jnp.where(down == iota((tok, tok), 1), 1.0, 0.0).astype(BF16)
    picked = dot(chosen, image)
    stitch_buf[p.high, p.core] = jnp.where(down[:, :1] >= 0, picked, text[...].astype(F32)).astype(BF16)
    stitch_gather.start()

    lane = iota((PAIR * tok, HD), 1)
    row = iota((PAIR * tok, HD), 0)
    step = (lane & (HD // 2 - 1)).astype(F32) * (2.0 / HD)
    first = (p.deep * WIDE + p.wide) * tok
    position = first + (row & (tok - 1)) + jnp.where(row >= tok, DEEP * WIDE * tok, 0)
    angle = position.astype(F32) * jnp.exp(-math.log(THETA) * step)
    cosine = jnp.cos(angle)
    sine = jnp.where(lane < HD // 2, -1.0, 1.0) * jnp.sin(angle)

    rest = list(range(7, DEEP + 2))
    for t in range(1, ROWS * PAIR):
        if rest and t % 2:
            at = rest.pop(0)
            weight_gather.step(p.pair, 0, at)
            weight_gather.step(1 - p.pair, 1, at)
        stitch_gather.step(t)
    for at in rest:
        weight_gather.step(p.pair, 0, at)
        weight_gather.step(1 - p.pair, 1, at)
    stitch_gather.finish()

    heads = ROWS * CORES
    scales = []
    for q in range(PAIR):
        square = jnp.zeros((tok, width), F32)
        for h in range(heads):
            block = stitch_buf[(h // CORES) * PAIR + q, h % CORES].astype(F32)
            square += block * block
        scales.append(lax.rsqrt(jnp.sum(square, axis=-1, keepdims=True) / (heads * width) + EPSILON))
    bias = qkv_bias[pl.ds(pl.multiple_of(p.pair * columns, 128), columns)].reshape(1, -1)
    projected = jnp.broadcast_to(bias, (PAIR * tok, columns))
    gains = line(llm_gain)
    span = width // w_qkv.shape[0] // WIDE
    for h in range(heads):
        gain = gains[:, h * width : (h + 1) * width]
        block = jnp.concatenate(
            [
                (stitch_buf[(h // CORES) * PAIR + q, h % CORES].astype(F32) * scales[q] * gain).astype(BF16)
                for q in range(PAIR)
            ],
            axis=0,
        )
        first = h * span
        rows = weight_buf[first // DEEP, first % DEEP : first % DEEP + span]
        projected += dot(block, rows.reshape(width, columns))
    for i in (2, 1, 0):
        value = projected[:, i * HD : (i + 1) * HD]
        plain = 3 * p.pair + i == QH + 1
        done = turn(value, jnp.where(plain, 1.0, cosine), jnp.where(plain, 0.0, sine)).astype(BF16)
        for q in range(PAIR):
            mine_buf[q, i] = done[q * tok : (q + 1) * tok]
    copies.send(
        lambda: mine_buf.at[1 - p.pair], swaps[2], p.other_pair, lambda: theirs_buf.at[...]
    )

    @pl.when(p.pair == 1)
    def _():
        for q in range(PAIR):
            kv_buf[q, p.deep, p.wide, :, :HD] = mine_buf[q, 1]
            kv_buf[q, p.deep, p.wide, :, HD:] = mine_buf[q, 2]
        for j in range(QH - 1, QH):
            query_buf[j * tok : (j + 1) * tok] = mine_buf[1, 0]
        kv_gather.start(1, 1)

    copies.wait(theirs_buf.at[...], swaps[2], p.other_pair())

    @pl.when(p.pair == 1)
    def _():
        for j in range(QH - 1):
            query_buf[j * tok : (j + 1) * tok] = theirs_buf[j]

    @pl.when(p.pair == 0)
    def _():
        kv_buf[0, p.deep, p.wide, :, :HD] = theirs_buf[1]
        kv_buf[0, p.deep, p.wide, :, HD:] = theirs_buf[2]
        for j in range(QH - 1):
            query_buf[j * tok : (j + 1) * tok] = mine_buf[0, j]
        query_buf[(QH - 1) * tok :] = theirs_buf[0]

    kv_gather.start(0, 0)
    group = p.pair * DEEP + p.deep
    state = (top_ref, total_ref, sum_ref, query_buf)
    for t in range(DEEP + 2):

        @pl.when(p.pair == 1)
        def _():
            kv_gather.step(1, 1, t)

        kv_gather.step(0, 0, t)
        if t == 2:
            shape = (QH * tok, WIDE * tok)
            rows, cols = iota(shape, 0), iota(shape, 1)
            allowed = cols <= p.wide * tok + (rows & (tok - 1))
            attend(*state, kv_buf[p.pair, p.deep], allowed)
        if t >= 2:
            deep = p.deep_at(kv_gather.offset(t - 2))

            def visit(pair, _):
                @pl.when(pair * DEEP + deep < group)
                def _():
                    attend(*state, kv_buf[pair, deep], None)

                return 0

            lax.fori_loop(0, 1 if t == 2 else PAIR, visit, 0)
    result = (sum_ref[...] / total_ref[...]).astype(BF16)
    for j in range(QH):
        out[:, j * HD : (j + 1) * HD] = result[j * tok : (j + 1) * tok]
    copies.drain(False)

    @pl.when(p.pair == 1)
    def _():
        copies.drain(True)


def body(
    patches,
    patch_count,
    token_patch,
    window_ids,
    text_embed,
    vit_norm_gain,
    vit_qkv,
    vit_qkv_bias,
    vit_proj,
    vit_proj_bias,
    merge_norm_gain,
    merger,
    merger_bias,
    llm_norm_gain,
    w_qkv,
    qkv_bias,
):
    tok = patches.shape[0]
    width = text_embed.shape[1]
    vmem = pl.BlockSpec(memory_space=pltpu.VMEM)
    hbm = pl.BlockSpec(memory_space=pltpu.HBM)
    specs = [vmem] * 16
    specs[8] = specs[14] = hbm
    ctx_shape = (PAIR, DEEP, WIDE)
    heads = ROWS * CORES
    plane = 2 * (WIDE - 1 + 2 * DEEP + DEEP * (WIDE - 1))
    slots = 3 + 3 * plane + 2 * ROWS + 13 + 4 * ROWS * PAIR
    parts = (3, tok, HD)
    return pl.pallas_call(
        kernel,
        out_shape=jax.ShapeDtypeStruct((tok, QH * HD), BF16),
        in_specs=specs,
        out_specs=vmem,
        scratch_shapes=[
            pltpu.VMEM(ctx_shape + (16, width + 128), BF16),
            pltpu.VMEM(ctx_shape + (w_qkv.shape[0], w_qkv.shape[1] // 2), BF16),
            pltpu.VMEM((heads,) + vit_proj.shape, BF16),
            pltpu.VMEM((heads, tok, vit_proj.shape[0]), BF16),
            pltpu.VMEM((ROWS * PAIR, CORES) + text_embed.shape, BF16),
            pltpu.VMEM((PAIR,) + parts, BF16),
            pltpu.VMEM(parts, BF16),
            pltpu.VMEM(ctx_shape + (tok, 2 * HD), BF16),
            pltpu.VMEM((QH * tok, HD), BF16),
            pltpu.VMEM((QH * tok, 1), F32),
            pltpu.VMEM((QH * tok, 1), F32),
            pltpu.VMEM((QH * tok, HD), F32),
            pltpu.SemaphoreType.DMA((2,)),
            pltpu.SemaphoreType.DMA((slots,)),
            pltpu.SemaphoreType.DMA((slots,)),
        ],
        compiler_params=pltpu.CompilerParams(
            collective_id=0, has_side_effects=True, vmem_limit_bytes=60 * 1024 * 1024
        ),
        name="whole",
    )(
        patches,
        patch_count.reshape(1, 1),
        token_patch,
        window_ids,
        text_embed,
        vit_norm_gain,
        vit_qkv.T,
        vit_qkv_bias,
        vit_proj,
        vit_proj_bias,
        merge_norm_gain,
        merger,
        merger_bias,
        llm_norm_gain,
        w_qkv,
        qkv_bias,
    )


def solution(mesh):
    return jax.shard_map(
        body,
        mesh=mesh,
        in_specs=(
            P("ctx", None),
            P("ctx"),
            P("ctx"),
            P("ctx"),
            P("ctx", "head"),
            P(),
            P(None, "head"),
            P("head"),
            P("head", None),
            P(),
            P(),
            P("ctx", "head"),
            P("head"),
            P(),
            P("ctx", "head"),
            P("head"),
        ),
        out_specs=P("ctx", "head"),
        check_vma=False,
    )
```
